32 devices in a mesh: dp: 8 (over z, x), tensor: 4 (over y, core).
Axes of the slice: x: 2, y: 2, z: 4, core: 2. Of those that a mesh axis runs over, the one named last changes fastest.
Arguments:
- hidden: bfloat16 [2048, 14336], P('dp', 'tensor'), parts along dimension 0, may hold values from -16 to 16
- signs: int32 [14336], P('tensor'), may hold values 0 or 1
- packed: int32 [14336, 512], P('tensor'), may hold values from -2147483648 to 2147483646
- group_scales: int32 [112, 4096], P('tensor'), may hold values from 1 to 16
- residual: bfloat16 [2048, 4096], P(('dp', 'tensor')), parts along dimension 0, may hold values from -16 to 16
Outputs:
- new_residual: bfloat16 [2048, 4096], P(('dp', 'tensor')), parts along dimension 0
- normed: bfloat16 [2048, 4096], P(('dp', 'tensor')), parts along dimension 0
The draws below stay inside these ranges and needn't reach their ends.
There are 8 independent parts, one for each index of `dp`. The reference program is written for one: setup_inputs(seed, part) draws one part's arguments, and reference() takes and returns one part's arrays. A program takes and returns all parts, laid end to end along the dimension named above; an argument that names none is the same for every part. Nothing has to cross between parts.
Inputs may be any that keep to these rules, and one draw needn't show every extreme that they name: `packed`: bits 4 k to 4 k + 3 of word j in row f hold the code of output feature k * 512 + j plus 8.
All inputs are finite; a program needn't handle non-finite values. No bound on the sum of `signs` on one device may be relied on, other than what follows from the above.
Results may differ from the reference program's by a relative error of at most 0.0054.
Values may be sent and summed in bfloat16 or wider, within the bound.
A program may use at most 256 MiB of HBM per device.

```python
import math
import jax
import jax.numpy as jnp
import numpy as np
from jax import lax

D = 4096
FF = 14336
GROUP = 128
ROWS = 256


def scaled_draw(key, count, width):
    first = jax.random.fold_in(key, 0)
    third = jax.random.fold_in(key, 2)
    column_scale = jnp.exp(jax.random.uniform(first, (1, width), jnp.float32, math.log(0.3), math.log(3.0)))
    values = jax.random.normal(third, (count, width), jnp.float32) * column_scale
    return jnp.clip(values, -16.0, 16.0)


def draw_hidden(key, part):
    return scaled_draw(jax.random.fold_in(key, 11), ROWS, FF).astype(jnp.bfloat16)


def draw_residual(key, part):
    return scaled_draw(jax.random.fold_in(key, 23), ROWS, D).astype(jnp.bfloat16)


def touch_ends(values, rng, low, high):
    spot = [jax.random.randint(jax.random.fold_in(rng, axis), (), 0, length) for axis, length in enumerate(values.shape)]
    main_axis = values.shape.index(max(values.shape))
    beside = spot[:main_axis] + [(spot[main_axis] + 1) % values.shape[main_axis]] + spot[main_axis + 1:]
    return values.at[tuple(spot)].set(low).at[tuple(beside)].set(high)


def setup_inputs(seed: int = 0, part: int = 0) -> dict:
    key_of = jax.random.split(jax.random.key(seed), 6)
    own_keys = jax.random.split(jax.random.fold_in(key_of[5], part), 6)
    hidden = draw_hidden(jax.random.fold_in(jax.random.fold_in(key_of[5], part), 71), part)
    signs = touch_ends((jax.random.randint(key_of[1], (FF,), 0, 2) < 1).astype(jnp.int32), jax.random.fold_in(key_of[1], 1), 0, 1)
    packed = touch_ends(jax.random.randint(key_of[2], (FF, D // 8), -2147483648, 2147483647), jax.random.fold_in(key_of[2], 1), -2147483648, 2147483646).astype(jnp.int32)
    group_scales = touch_ends(jax.random.randint(key_of[3], (FF // GROUP, D), 1, 17), jax.random.fold_in(key_of[3], 1), 1, 16).astype(jnp.int32)
    residual = draw_residual(jax.random.fold_in(jax.random.fold_in(key_of[5], part), 71), part)
    return {"hidden": hidden, "signs": signs, "packed": packed, "group_scales": group_scales, "residual": residual}


def paley_table():
    offsets = (np.arange(13)[None, :] - np.arange(13)[:, None]) % 13
    residues = np.zeros(13)
    residues[np.arange(1, 13) ** 2 % 13] = 1.0
    quadratic = np.where(offsets == 0, 0.0, np.where(residues[offsets] > 0, 1.0, -1.0))
    conference = np.zeros((14, 14))
    conference[0, 1:] = 1.0
    conference[1:, 0] = 1.0
    conference[1:, 1:] = quadratic
    upper = np.array([[1.0, 1.0], [1.0, -1.0]])
    lower = np.array([[1.0, -1.0], [-1.0, -1.0]])
    return np.kron(conference, upper) + np.kron(np.eye(14), lower)

def sylvester(order):
    first = lax.broadcasted_iota(jnp.int32, (order, order), 0)
    second = lax.broadcasted_iota(jnp.int32, (order, order), 1)
    common = first & second
    parity = jnp.zeros((order, order), jnp.int32)
    for bit in range(max(order.bit_length() - 1, 0)):
        parity = parity ^ jnp.right_shift(common, bit) & 1
    return (1 - 2 * parity).astype(jnp.float32)

def reference(hidden, signs, packed, group_scales, residual):
    count = hidden.shape[0]
    flips = (2 * signs - 1).astype(jnp.float32)
    signed = hidden.astype(jnp.float32) * flips[None, :]
    blocks = signed.reshape(count, FF // 28, 28)
    outer = sylvester(FF // 28)
    inner = jnp.asarray(paley_table(), jnp.float32)
    mixed = jnp.einsum('rba,cb->rca', blocks, outer, precision=lax.Precision.HIGHEST)
    mixed = jnp.einsum('rca,da->rcd', mixed, inner, precision=lax.Precision.HIGHEST)
    rotated = (mixed.reshape(count, FF) * (1.0 / math.sqrt(FF))).astype(jnp.bfloat16)
    width = D // 8
    pieces = []
    for nibble in range(8):
        codes = (jnp.right_shift(packed, 4 * nibble) & 15) - 8
        scales = group_scales[:, nibble * width:(nibble + 1) * width]
        weights = (codes.reshape(FF // GROUP, GROUP, width) * scales[:, None, :]).reshape(FF, width)
        pieces.append(jnp.dot(rotated, weights.astype(jnp.bfloat16), preferred_element_type=jnp.float32))
    branch = jnp.concatenate(pieces, axis=1) * (1.0 / (45.0 * math.sqrt(FF)))
    new_residual = (residual.astype(jnp.float32) + branch).astype(jnp.bfloat16)
    values = new_residual.astype(jnp.float32)
    normed = values * lax.rsqrt(lax.optimization_barrier(jnp.mean(values * values, axis=1, keepdims=True)) + 1e-05)
    return (new_residual, normed.astype(jnp.bfloat16))
```

```python
import functools
import math

import jax
import jax.numpy as jnp
import ml_dtypes
import numpy as np
from jax import lax
from jax.experimental import pallas as pl
from jax.experimental.pallas import tpu as pltpu
from jax.sharding import PartitionSpec as P

PALEY = 28
LANES = 128
NIBBLES = 8
SLAB = 16
MESH = pl.DeviceIdType.MESH


def paley_table():
    offsets = (np.arange(13)[None, :] - np.arange(13)[:, None]) % 13
    residues = np.zeros(13)
    residues[np.arange(1, 13) ** 2 % 13] = 1.0
    quadratic = np.where(offsets == 0, 0.0, np.where(residues[offsets] > 0, 1.0, -1.0))
    conference = np.zeros((14, 14))
    conference[0, 1:] = 1.0
    conference[1:, 0] = 1.0
    conference[1:, 1:] = quadratic
    upper = np.array([[1.0, 1.0], [1.0, -1.0]])
    lower = np.array([[1.0, -1.0], [-1.0, -1.0]])
    return np.kron(conference, upper) + np.kron(np.eye(14), lower)


def sylvester(order):
    table = np.ones((1, 1))
    while table.shape[0] < order:
        table = np.kron(np.array([[1.0, 1.0], [1.0, -1.0]]), table)
    return table


def parity_sign(index, other, bits):
    common = index & other
    parity = common & 1
    for bit in range(1, bits):
        parity = parity ^ ((common >> bit) & 1)
    return (1 - 2 * parity).astype(jnp.float32)


def kernel(
    groups,
    signed,
    packed,
    scales,
    table,
    residual,
    new_residual,
    normed,
    words,
    inner,
    gathered,
    scale_f32,
    weights,
    rotated,
    sums,
    own,
    core_out,
    core_in,
    chip_out,
    chip_in,
    word_sem,
    inner_sem,
    self_sem,
    peer_send,
    peer_recv,
    core_send,
    core_recv,
    fold_send,
    fold_recv,
    chip_send,
    chip_recv,
):
    me = lax.axis_index("tensor")
    chips = groups // 2
    chip, core = me // 2, lax.rem(me, 2)
    partner = chip * 2 + 1 - core
    rows, width = signed.shape
    part = rows // groups
    group_count = scales.shape[0]
    group_size = width // group_count
    word_cols = packed.shape[1]
    block = table.shape[0]
    blocks = width // block
    bits = max(groups.bit_length() - 1, 1)

    word_copies = [
        pltpu.make_async_copy(packed, words, word_sem),
        pltpu.make_async_copy(table, inner, inner_sem),
        pltpu.make_async_copy(signed, gathered.at[me], self_sem),
    ]
    for copy in word_copies:
        copy.start()

    def peer(step):
        return lax.rem(chip + step, chips) * 2 + core

    barrier = pltpu.get_barrier_semaphore()
    pl.semaphore_signal(barrier, inc=1, device_id={"tensor": partner}, device_id_type=MESH)
    for step in range(1, chips):
        pl.semaphore_signal(barrier, inc=1, device_id={"tensor": peer(step)}, device_id_type=MESH)
    pl.semaphore_wait(barrier, chips)

    def band(index):
        return pl.ds(pl.multiple_of(index * part, part), part)

    def peer_copy(step, piece):
        return pltpu.make_async_remote_copy(
            src_ref=signed.at[band(piece)],
            dst_ref=gathered.at[me, band(piece)],
            send_sem=peer_send.at[step, piece],
            recv_sem=peer_recv.at[step, piece],
            device_id={"tensor": peer(step)},
            device_id_type=MESH,
        )

    def core_copy(step, piece):
        source = signed.at[band(piece)] if step == 0 else gathered.at[peer(chips - step), band(piece)]
        slot = me if step == 0 else peer(chips - step)
        return pltpu.make_async_remote_copy(
            src_ref=source,
            dst_ref=gathered.at[slot, band(piece)],
            send_sem=core_send.at[step, piece],
            recv_sem=core_recv.at[step, piece],
            device_id={"tensor": partner},
            device_id_type=MESH,
        )

    for piece in range(groups):
        for step in range(1, chips):
            peer_copy(step, piece).start()
        core_copy(0, piece).start()

    scale_f32[...] = scales[...].astype(jnp.float32)
    word_copies[0].wait()

    def dequantize(index, carry):
        start = pl.multiple_of(index * SLAB, SLAB)
        group = index // (group_size // SLAB)
        values = words[pl.ds(start, SLAB), :] ^ jnp.int32(-2004318072)
        for nibble in range(NIBBLES):
            codes = lax.shift_right_arithmetic(lax.shift_left(values, 28 - 4 * nibble), 28)
            scale = scale_f32[pl.ds(group, 1), nibble * word_cols : (nibble + 1) * word_cols]
            weights[nibble, pl.ds(start, SLAB), :] = (codes.astype(jnp.float32) * scale).astype(jnp.bfloat16)
        return carry

    lax.fori_loop(0, width // SLAB, dequantize, 0)
    word_copies[1].wait()
    word_copies[2].wait()

    unit = 1.0 / math.sqrt(groups * width)
    outer = sylvester(blocks)

    def rotate(piece, carry):
        for step in range(1, chips):
            peer_copy(step, piece).wait_recv()
            core_copy(step, piece).start()
        for step in range(chips):
            core_copy(step, piece).wait_recv()
        mixed = []
        for place in range(blocks):
            total = jnp.zeros((part, block), jnp.float32)
            for device in range(groups):
                sign = parity_sign(me, device, bits)
                total += gathered[device, band(piece), place * block : (place + 1) * block].astype(jnp.float32) * sign
            high = total.astype(jnp.bfloat16)
            low = (total - high.astype(jnp.float32)).astype(jnp.bfloat16)
            both = jnp.dot(jnp.concatenate([high, low], axis=0), inner[...], preferred_element_type=jnp.float32)
            mixed.append(both[:part] + both[part:])
        stride = 1
        while stride < blocks:
            for low_index in range(blocks):
                if low_index & stride == 0:
                    first, second = mixed[low_index], mixed[low_index + stride]
                    mixed[low_index], mixed[low_index + stride] = first + second, first - second
            stride *= 2
        for place in range(blocks):
            rotated[band(piece), place * block : (place + 1) * block] = (mixed[place] * unit).astype(jnp.bfloat16)
        return carry

    lax.fori_loop(0, groups, rotate, 0)

    def fold_copy(column):
        return pltpu.make_async_remote_copy(
            src_ref=core_out.at[column],
            dst_ref=core_in.at[column],
            send_sem=fold_send.at[column],
            recv_sem=fold_recv.at[column],
            device_id={"tensor": partner},
            device_id_type=MESH,
        )

    def chip_copy(step, column):
        return pltpu.make_async_remote_copy(
            src_ref=chip_out.at[column, step],
            dst_ref=chip_in.at[column, step],
            send_sem=chip_send.at[step, column],
            recv_sem=chip_recv.at[step, column],
            device_id={"tensor": peer(step)},
            device_id_type=MESH,
        )

    def multiply(column):
        sums[...] = jnp.dot(rotated[...], weights[column], preferred_element_type=jnp.float32)
        for step in range(chips):
            target = lax.rem(chip + step, chips)
            core_out[column, target] = sums[band(target * 2 + 1 - core), :].astype(jnp.bfloat16)
            own[column, step] = sums[band(target * 2 + core), :]
        fold_copy(column).start()

    def fold(column):
        fold_copy(column).wait_recv()
        for step in range(1, chips):
            target = lax.rem(chip + step, chips)
            chip_out[column, step] = (
                own[column, step] + core_in[column, target].astype(jnp.float32)
            ).astype(jnp.bfloat16)
            chip_copy(step, column).start()
        own[column, 0] = own[column, 0] + core_in[column, chip].astype(jnp.float32)

    def column_step(column, carry):
        multiply(column)

        @pl.when(column > 0)
        def _():
            fold(column - 1)

        return carry

    lax.fori_loop(0, NIBBLES, column_step, 0)
    fold(NIBBLES - 1)

    factor = 1.0 / (45.0 * math.sqrt(groups * width))
    squares = jnp.zeros((part, 1), jnp.float32)
    for column in range(NIBBLES):
        span = slice(column * word_cols, (column + 1) * word_cols)
        total = own[column, 0]
        for step in range(1, chips):
            chip_copy(step, column).wait_recv()
            total += chip_in[column, step].astype(jnp.float32)
        fresh = (residual[:, span].astype(jnp.float32) + total * factor).astype(jnp.bfloat16)
        new_residual[:, span] = fresh
        values = fresh.astype(jnp.float32)
        squares += jnp.sum(values * values, axis=1, keepdims=True)
    inverse = lax.rsqrt(squares * (1.0 / (NIBBLES * word_cols)) + 1e-05)
    for column in range(NIBBLES):
        span = slice(column * word_cols, (column + 1) * word_cols)
        normed[:, span] = (new_residual[:, span].astype(jnp.float32) * inverse).astype(jnp.bfloat16)

    def drain_rows(piece, carry):
        for step in range(1, chips):
            peer_copy(step, piece).wait_send()
        for step in range(chips):
            core_copy(step, piece).wait_send()
        return carry

    lax.fori_loop(0, groups, drain_rows, 0)

    def drain_columns(column, carry):
        fold_copy(column).wait_send()
        for step in range(1, chips):
            chip_copy(step, column).wait_send()
        return carry

    lax.fori_loop(0, NIBBLES, drain_columns, 0)


def local(groups, hidden, signs, packed, group_scales, residual):
    rows, width = hidden.shape
    part = rows // groups
    chips = groups // 2
    word_cols = packed.shape[1]
    block = math.lcm(PALEY, LANES)
    table = np.kron(sylvester(block // PALEY), paley_table()).astype(ml_dtypes.bfloat16)
    signed = hidden * (2 * signs - 1).astype(jnp.bfloat16)[None, :]
    vmem = pl.BlockSpec(memory_space=pltpu.VMEM)
    anywhere = pl.BlockSpec(memory_space=pl.ANY)
    dma = pltpu.SemaphoreType.DMA
    tall = (NIBBLES, chips, part, word_cols)
    return pl.pallas_call(
        functools.partial(kernel, groups),
        out_shape=(
            jax.ShapeDtypeStruct(residual.shape, jnp.bfloat16),
            jax.ShapeDtypeStruct(residual.shape, jnp.bfloat16),
        ),
        in_specs=[anywhere, anywhere, vmem, anywhere, vmem],
        out_specs=(vmem, vmem),
        scratch_shapes=[
            pltpu.VMEM(packed.shape, jnp.int32),
            pltpu.VMEM((block, block), jnp.bfloat16),
            pltpu.VMEM((groups, rows, width), jnp.bfloat16),
            pltpu.VMEM(group_scales.shape, jnp.float32),
            pltpu.VMEM((NIBBLES, width, word_cols), jnp.bfloat16),
            pltpu.VMEM((rows, width), jnp.bfloat16),
            pltpu.VMEM((rows, word_cols), jnp.float32),
            pltpu.VMEM(tall, jnp.float32),
            pltpu.VMEM(tall, jnp.bfloat16),
            pltpu.VMEM(tall, jnp.bfloat16),
            pltpu.VMEM(tall, jnp.bfloat16),
            pltpu.VMEM(tall, jnp.bfloat16),
            dma,
            dma,
            dma,
            dma((chips, groups)),
            dma((chips, groups)),
            dma((chips, groups)),
            dma((chips, groups)),
            dma((NIBBLES,)),
            dma((NIBBLES,)),
            dma((chips, NIBBLES)),
            dma((chips, NIBBLES)),
        ],
        compiler_params=pltpu.CompilerParams(
            collective_id=0, has_side_effects=True, vmem_limit_bytes=67043328
        ),
    )(signed, packed, group_scales, jnp.asarray(table), residual)


def solution(mesh):
    return jax.shard_map(
        functools.partial(local, mesh.shape["tensor"]),
        mesh=mesh,
        in_specs=(
            P("dp", "tensor"),
            P("tensor"),
            P("tensor", None),
            P("tensor", None),
            P(("dp", "tensor"), None),
        ),
        out_specs=(P(("dp", "tensor"), None), P(("dp", "tensor"), None)),
        check_vma=False,
    )
```

```python
import functools
import math

import jax
import jax.numpy as jnp
import ml_dtypes
import numpy as np
from jax import lax
from jax.experimental import pallas as pl
from jax.experimental.pallas import tpu as pltpu
from jax.sharding import PartitionSpec as P

PALEY = 28
LANES = 128
NIBBLES = 8
SLAB = 16
WAVES = 2
MESH = pl.DeviceIdType.MESH


def paley_table():
    offsets = (np.arange(13)[None, :] - np.arange(13)[:, None]) % 13
    residues = np.zeros(13)
    residues[np.arange(1, 13) ** 2 % 13] = 1.0
    quadratic = np.where(offsets == 0, 0.0, np.where(residues[offsets] > 0, 1.0, -1.0))
    conference = np.zeros((14, 14))
    conference[0, 1:] = 1.0
    conference[1:, 0] = 1.0
    conference[1:, 1:] = quadratic
    upper = np.array([[1.0, 1.0], [1.0, -1.0]])
    lower = np.array([[1.0, -1.0], [-1.0, -1.0]])
    return np.kron(conference, upper) + np.kron(np.eye(14), lower)


def sylvester(order):
    table = np.ones((1, 1))
    while table.shape[0] < order:
        table = np.kron(np.array([[1.0, 1.0], [1.0, -1.0]]), table)
    return table


def parity_sign(index, other, bits):
    common = index & other
    parity = common & 1
    for bit in range(1, bits):
        parity = parity ^ ((common >> bit) & 1)
    return (1 - 2 * parity).astype(jnp.float32)


def kernel(
    groups,
    waves,
    hidden,
    signs,
    packed,
    scales,
    table,
    residual,
    new_residual,
    words,
    inner,
    gathered,
    bits_in,
    flips,
    scale_f32,
    weights,
    rotated,
    sums,
    own,
    core_out,
    core_in,
    chip_out,
    chip_in,
    word_sem,
    inner_sem,
    self_sem,
    sign_send,
    sign_recv,
    peer_send,
    peer_recv,
    core_send,
    core_recv,
    fold_send,
    fold_recv,
    chip_send,
    chip_recv,
):
    me = lax.axis_index("tensor")
    chips = groups // 2
    chip, core = me // 2, lax.rem(me, 2)
    partner = chip * 2 + 1 - core
    part, width = hidden.shape[1:]
    sub = part // waves
    units = groups // waves
    group_count = scales.shape[0]
    group_size = width // group_count
    word_cols = packed.shape[1]
    block = table.shape[0]
    blocks = width // block
    bits = max(groups.bit_length() - 1, 1)

    word_copies = [
        pltpu.make_async_copy(packed, words, word_sem),
        pltpu.make_async_copy(table, inner, inner_sem),
        pltpu.make_async_copy(hidden, gathered.at[me], self_sem),
    ]
    for copy in word_copies:
        copy.start()

    def peer(step):
        return lax.rem(chip + step, chips) * 2 + core

    barrier = pltpu.get_barrier_semaphore()
    for step in range(1, groups):
        other = lax.rem(me + step, groups)
        pl.semaphore_signal(barrier, inc=1, device_id={"tensor": other}, device_id_type=MESH)
    pl.semaphore_wait(barrier, groups - 1)

    def sign_copy(step):
        return pltpu.make_async_remote_copy(
            src_ref=signs,
            dst_ref=bits_in.at[me],
            send_sem=sign_send.at[step],
            recv_sem=sign_recv.at[step],
            device_id={"tensor": lax.rem(me + step, groups)},
            device_id_type=MESH,
        )

    def place_of(unit):
        return pl.ds(lax.rem(unit, units) * waves, waves), pl.ds(pl.multiple_of(unit // units * sub, sub), sub)

    def peer_copy(step, unit):
        return pltpu.make_async_remote_copy(
            src_ref=hidden.at[place_of(unit)],
            dst_ref=gathered.at[(me,) + place_of(unit)],
            send_sem=peer_send.at[step, unit],
            recv_sem=peer_recv.at[step, unit],
            device_id={"tensor": peer(step)},
            device_id_type=MESH,
        )

    def core_copy(step, unit):
        slot = me if step == 0 else peer(chips - step)
        source = hidden.at[place_of(unit)] if step == 0 else gathered.at[(slot,) + place_of(unit)]
        return pltpu.make_async_remote_copy(
            src_ref=source,
            dst_ref=gathered.at[(slot,) + place_of(unit)],
            send_sem=core_send.at[step, unit],
            recv_sem=core_recv.at[step, unit],
            device_id={"tensor": partner},
            device_id_type=MESH,
        )

    for step in range(1, groups):
        sign_copy(step).start()
    for unit in range(groups):
        for step in range(1, chips):
            peer_copy(step, unit).start()
        core_copy(0, unit).start()

    scale_f32[...] = scales[...].astype(jnp.float32)
    word_copies[0].wait()

    def dequantize(index, carry):
        start = pl.multiple_of(index * SLAB, SLAB)
        group = index // (group_size // SLAB)
        values = words[pl.ds(start, SLAB), :] ^ jnp.int32(-2004318072)
        for nibble in range(NIBBLES):
            codes = lax.shift_right_arithmetic(lax.shift_left(values, 28 - 4 * nibble), 28)
            scale = scale_f32[pl.ds(group, 1), nibble * word_cols : (nibble + 1) * word_cols]
            weights[nibble, pl.ds(start, SLAB), :] = (codes.astype(jnp.float32) * scale).astype(jnp.bfloat16)
        return carry

    lax.fori_loop(0, width // SLAB, dequantize, 0)
    word_copies[1].wait()
    word_copies[2].wait()
    for step in range(1, groups):
        sign_copy(step).wait_recv()
    for step in range(groups):
        device = lax.rem(me + step, groups)
        source = signs if step == 0 else bits_in.at[device]
        flips[device] = (2 * source[...] - 1).astype(jnp.float32) * parity_sign(me, device, bits)

    scale_unit = 1.0 / math.sqrt(groups * width)

    def rotate(unit, carry):
        for step in range(1, chips):
            peer_copy(step, unit).wait_recv()
            core_copy(step, unit).start()
        for step in range(chips):
            core_copy(step, unit).wait_recv()
        mixed = []
        for place in range(blocks):
            total = jnp.zeros((part, block), jnp.float32)
            for device in range(groups):
                piece = gathered[(device,) + place_of(unit) + (pl.ds(place * block, block),)]
                first_row = place * block // LANES
                flip = jnp.concatenate(
                    [flips[device, pl.ds(first_row + i, 1), :] for i in range(block // LANES)], axis=1
                )
                total += piece.reshape(part, block).astype(jnp.float32) * flip
            high = total.astype(jnp.bfloat16)
            low = (total - high.astype(jnp.float32)).astype(jnp.bfloat16)
            both = jnp.dot(jnp.concatenate([high, low], axis=0), inner[...], preferred_element_type=jnp.float32)
            mixed.append(both[:part] + both[part:])
        stride = 1
        while stride < blocks:
            for low_index in range(blocks):
                if low_index & stride == 0:
                    first, second = mixed[low_index], mixed[low_index + stride]
                    mixed[low_index], mixed[low_index + stride] = first + second, first - second
            stride *= 2
        for place in range(blocks):
            rotated[unit // units, pl.ds(pl.multiple_of(lax.rem(unit, units) * part, part), part), place * block : (place + 1) * block] = (
                mixed[place] * scale_unit
            ).astype(jnp.bfloat16)
        return carry

    def band(index):
        return pl.ds(pl.multiple_of(index * sub, sub), sub)

    def fold_copy(column):
        return pltpu.make_async_remote_copy(
            src_ref=core_out.at[column],
            dst_ref=core_in.at[column],
            send_sem=fold_send.at[column],
            recv_sem=fold_recv.at[column],
            device_id={"tensor": partner},
            device_id_type=MESH,
        )

    def chip_copy(step, column):
        return pltpu.make_async_remote_copy(
            src_ref=chip_out.at[column, step],
            dst_ref=chip_in.at[column, step],
            send_sem=chip_send.at[step, column],
            recv_sem=chip_recv.at[step, column],
            device_id={"tensor": peer(step)},
            device_id_type=MESH,
        )

    def multiply(column):
        wave, nibble = column // NIBBLES, lax.rem(column, NIBBLES)
        sums[...] = jnp.dot(rotated[wave], weights[nibble], preferred_element_type=jnp.float32)
        for step in range(chips):
            target = lax.rem(chip + step, chips)
            core_out[column, target] = sums[band(target * 2 + 1 - core), :].astype(jnp.bfloat16)
            own[column, step] = sums[band(target * 2 + core), :]
        fold_copy(column).start()

    def fold(column):
        fold_copy(column).wait_recv()
        for step in range(1, chips):
            target = lax.rem(chip + step, chips)
            chip_out[column, step] = (
                own[column, step] + core_in[column, target].astype(jnp.float32)
            ).astype(jnp.bfloat16)
            chip_copy(step, column).start()
        own[column, 0] = own[column, 0] + core_in[column, chip].astype(jnp.float32)

    def column_step(column, carry):
        multiply(column)

        @pl.when(column > 0)
        def _():
            fold(column - 1)

        return carry

    for wave in range(waves):
        lax.fori_loop(wave * units, (wave + 1) * units, rotate, 0)
        lax.fori_loop(wave * NIBBLES, (wave + 1) * NIBBLES, column_step, 0)
    fold(waves * NIBBLES - 1)

    factor = 1.0 / (45.0 * math.sqrt(groups * width))
    for column in range(waves * NIBBLES):
        wave, nibble = column // NIBBLES, column % NIBBLES
        span = (slice(wave * sub, (wave + 1) * sub), slice(nibble * word_cols, (nibble + 1) * word_cols))
        total = own[column, 0]
        for step in range(1, chips):
            chip_copy(step, column).wait_recv()
            total += chip_in[column, step].astype(jnp.float32)
        new_residual[span] = (residual[span].astype(jnp.float32) + total * factor).astype(jnp.bfloat16)

    def drain_rows(unit, carry):
        for step in range(1, chips):
            peer_copy(step, unit).wait_send()
        for step in range(chips):
            core_copy(step, unit).wait_send()
        return carry

    for step in range(1, groups):
        sign_copy(step).wait_send()
    lax.fori_loop(0, groups, drain_rows, 0)

    def drain_columns(column, carry):
        fold_copy(column).wait_send()
        for step in range(1, chips):
            chip_copy(step, column).wait_send()
        return carry

    lax.fori_loop(0, waves * NIBBLES, drain_columns, 0)


def finish(fresh, new_residual, normed):
    values = fresh[...].astype(jnp.float32)
    new_residual[...] = fresh[...]
    inverse = lax.rsqrt(jnp.mean(values * values, axis=1, keepdims=True) + 1e-05)
    normed[...] = (values * inverse).astype(jnp.bfloat16)


def local(groups, hidden, signs, packed, group_scales, residual):
    rows, width = hidden.shape
    part = rows // groups
    chips = groups // 2
    waves = max(1, min(WAVES, part // SLAB, groups))
    word_cols = packed.shape[1]
    block = math.lcm(PALEY, LANES)
    table = np.kron(sylvester(block // PALEY), paley_table()).astype(ml_dtypes.bfloat16)
    vmem = pl.BlockSpec(memory_space=pltpu.VMEM)
    anywhere = pl.BlockSpec(memory_space=pl.ANY)
    dma = pltpu.SemaphoreType.DMA
    count = waves * NIBBLES
    tall = (count, chips, part // waves, word_cols)
    sign_shape = (width // LANES, LANES)
    out = jax.ShapeDtypeStruct(residual.shape, jnp.bfloat16)
    fresh = pl.pallas_call(
        functools.partial(kernel, groups, waves),
        out_shape=out,
        in_specs=[anywhere, vmem, anywhere, vmem, anywhere, vmem],
        out_specs=vmem,
        scratch_shapes=[
            pltpu.VMEM(packed.shape, jnp.int32),
            pltpu.VMEM((block, block), jnp.bfloat16),
            pltpu.VMEM((groups, groups, part, width), jnp.bfloat16),
            pltpu.VMEM((groups,) + sign_shape, jnp.int32),
            pltpu.VMEM((groups,) + sign_shape, jnp.float32),
            pltpu.VMEM(group_scales.shape, jnp.float32),
            pltpu.VMEM((NIBBLES, width, word_cols), jnp.bfloat16),
            pltpu.VMEM((waves, rows // waves, width), jnp.bfloat16),
            pltpu.VMEM((rows // waves, word_cols), jnp.float32),
            pltpu.VMEM(tall, jnp.float32),
            pltpu.VMEM(tall, jnp.bfloat16),
            pltpu.VMEM(tall, jnp.bfloat16),
            pltpu.VMEM(tall, jnp.bfloat16),
            pltpu.VMEM(tall, jnp.bfloat16),
            dma,
            dma,
            dma,
            dma((groups,)),
            dma((groups,)),
            dma((chips, groups)),
            dma((chips, groups)),
            dma((chips, groups)),
            dma((chips, groups)),
            dma((count,)),
            dma((count,)),
            dma((chips, count)),
            dma((chips, count)),
        ],
        compiler_params=pltpu.CompilerParams(
            collective_id=0, has_side_effects=True, vmem_limit_bytes=67043328
        ),
    )(
        hidden.reshape(groups, part, width),
        signs.reshape(sign_shape),
        packed,
        group_scales,
        jnp.asarray(table),
        residual,
    )
    return pl.pallas_call(
        finish,
        out_shape=(out, out),
        in_specs=[vmem],
        out_specs=(vmem, vmem),
    )(fresh)


def solution(mesh):
    return jax.shard_map(
        functools.partial(local, mesh.shape["tensor"]),
        mesh=mesh,
        in_specs=(
            P("dp", "tensor"),
            P("tensor"),
            P("tensor", None),
            P("tensor", None),
            P(("dp", "tensor"), None),
        ),
        out_specs=(P(("dp", "tensor"), None), P(("dp", "tensor"), None)),
        check_vma=False,
    )
```

```python
import functools
import math

import jax
import jax.numpy as jnp
import ml_dtypes
import numpy as np
from jax import lax
from jax.experimental import pallas as pl
from jax.experimental.pallas import tpu as pltpu
from jax.sharding import PartitionSpec as P

PALEY = 28
LANES = 128
NIBBLES = 8
SLAB = 16
WAVES = 2
MESH = pl.DeviceIdType.MESH


def paley_table():
    offsets = (np.arange(13)[None, :] - np.arange(13)[:, None]) % 13
    residues = np.zeros(13)
    residues[np.arange(1, 13) ** 2 % 13] = 1.0
    quadratic = np.where(offsets == 0, 0.0, np.where(residues[offsets] > 0, 1.0, -1.0))
    conference = np.zeros((14, 14))
    conference[0, 1:] = 1.0
    conference[1:, 0] = 1.0
    conference[1:, 1:] = quadratic
    upper = np.array([[1.0, 1.0], [1.0, -1.0]])
    lower = np.array([[1.0, -1.0], [-1.0, -1.0]])
    return np.kron(conference, upper) + np.kron(np.eye(14), lower)


def sylvester(order):
    table = np.ones((1, 1))
    while table.shape[0] < order:
        table = np.kron(np.array([[1.0, 1.0], [1.0, -1.0]]), table)
    return table


def parity_sign(index, other, bits):
    common = index & other
    parity = common & 1
    for bit in range(1, bits):
        parity = parity ^ ((common >> bit) & 1)
    return (1 - 2 * parity).astype(jnp.float32)


def kernel(
    groups,
    waves,
    hidden,
    signs,
    packed,
    scales_any,
    table,
    residual_any,
    new_residual,
    scales,
    residual,
    words,
    inner,
    gathered,
    bits_in,
    flips,
    scale_f32,
    weights,
    rotated,
    sums,
    own,
    core_out,
    core_in,
    chip_out,
    chip_in,
    word_sem,
    inner_sem,
    self_sem,
    flip_sem,
    scale_sem,
    residual_sem,
    sign_send,
    sign_recv,
    peer_send,
    peer_recv,
    core_send,
    core_recv,
    fold_send,
    fold_recv,
    chip_send,
    chip_recv,
):
    me = lax.axis_index("tensor")
    chips = groups // 2
    chip, core = me // 2, lax.rem(me, 2)
    partner = chip * 2 + 1 - core
    part, width = hidden.shape[1:]
    sub = part // waves
    units = groups // waves
    group_count = scales.shape[0]
    group_size = width // group_count
    word_cols = packed.shape[1]
    block = table.shape[0]
    blocks = width // block
    bits = max(groups.bit_length() - 1, 1)

    word_copies = [
        pltpu.make_async_copy(packed, words, word_sem),
        pltpu.make_async_copy(table, inner, inner_sem),
        pltpu.make_async_copy(hidden, gathered.at[me], self_sem),
        pltpu.make_async_copy(signs, bits_in.at[me], flip_sem),
        pltpu.make_async_copy(scales_any, scales, scale_sem),
        pltpu.make_async_copy(residual_any, residual, residual_sem),
    ]
    def peer(step):
        return lax.rem(chip + step, chips) * 2 + core

    barrier = pltpu.get_barrier_semaphore()
    for step in range(1, groups):
        other = lax.rem(me + step, groups)
        pl.semaphore_signal(barrier, inc=1, device_id={"tensor": other}, device_id_type=MESH)
    pl.semaphore_wait(barrier, groups - 1)

    def sign_copy(step):
        return pltpu.make_async_remote_copy(
            src_ref=signs,
            dst_ref=bits_in.at[me],
            send_sem=sign_send.at[step],
            recv_sem=sign_recv.at[step],
            device_id={"tensor": lax.rem(me + step, groups)},
            device_id_type=MESH,
        )

    def place_of(unit):
        return pl.ds(lax.rem(unit, units) * waves, waves), pl.ds(pl.multiple_of(unit // units * sub, sub), sub)

    def peer_copy(step, unit):
        return pltpu.make_async_remote_copy(
            src_ref=hidden.at[place_of(unit)],
            dst_ref=gathered.at[(me,) + place_of(unit)],
            send_sem=peer_send.at[step, unit],
            recv_sem=peer_recv.at[step, unit],
            device_id={"tensor": peer(step)},
            device_id_type=MESH,
        )

    def core_copy(step, unit):
        slot = me if step == 0 else peer(chips - step)
        source = hidden.at[place_of(unit)] if step == 0 else gathered.at[(slot,) + place_of(unit)]
        return pltpu.make_async_remote_copy(
            src_ref=source,
            dst_ref=gathered.at[(slot,) + place_of(unit)],
            send_sem=core_send.at[step, unit],
            recv_sem=core_recv.at[step, unit],
            device_id={"tensor": partner},
            device_id_type=MESH,
        )

    for step in range(1, groups):
        sign_copy(step).start()
    for unit in range(groups):
        for step in range(1, chips):
            peer_copy(step, unit).start()
        core_copy(0, unit).start()

    for copy in word_copies:
        copy.start()

    word_copies[4].wait()
    scale_f32[...] = scales[...].astype(jnp.float32)
    word_copies[0].wait()

    def dequantize(index, carry):
        start = pl.multiple_of(index * SLAB, SLAB)
        group = index // (group_size // SLAB)
        values = words[pl.ds(start, SLAB), :] ^ jnp.int32(-2004318072)
        for nibble in range(NIBBLES):
            codes = lax.shift_right_arithmetic(lax.shift_left(values, 28 - 4 * nibble), 28)
            scale = scale_f32[pl.ds(group, 1), nibble * word_cols : (nibble + 1) * word_cols]
            weights[nibble, pl.ds(start, SLAB), :] = (codes.astype(jnp.float32) * scale).astype(jnp.bfloat16)
        return carry

    lax.fori_loop(0, width // SLAB, dequantize, 0)
    word_copies[1].wait()
    word_copies[2].wait()
    word_copies[3].wait()
    word_copies[5].wait()
    for step in range(1, groups):
        sign_copy(step).wait_recv()
    for step in range(groups):
        device = lax.rem(me + step, groups)
        flips[device] = (2 * bits_in[device] - 1).astype(jnp.float32) * parity_sign(me, device, bits)

    scale_unit = 1.0 / math.sqrt(groups * width)

    def rotate(unit, carry):
        for step in range(1, chips):
            peer_copy(step, unit).wait_recv()
            core_copy(step, unit).start()
        for step in range(chips):
            core_copy(step, unit).wait_recv()
        mixed = []
        for place in range(blocks):
            total = jnp.zeros((part, block), jnp.float32)
            for device in range(groups):
                piece = gathered[(device,) + place_of(unit) + (pl.ds(place * block, block),)]
                first_row = place * block // LANES
                flip = jnp.concatenate(
                    [flips[device, pl.ds(first_row + i, 1), :] for i in range(block // LANES)], axis=1
                )
                total += piece.reshape(part, block).astype(jnp.float32) * flip
            high = total.astype(jnp.bfloat16)
            low = (total - high.astype(jnp.float32)).astype(jnp.bfloat16)
            both = jnp.dot(jnp.concatenate([high, low], axis=0), inner[...], preferred_element_type=jnp.float32)
            mixed.append(both[:part] + both[part:])
        stride = 1
        while stride < blocks:
            for low_index in range(blocks):
                if low_index & stride == 0:
                    first, second = mixed[low_index], mixed[low_index + stride]
                    mixed[low_index], mixed[low_index + stride] = first + second, first - second
            stride *= 2
        for place in range(blocks):
            rotated[unit // units, pl.ds(pl.multiple_of(lax.rem(unit, units) * part, part), part), place * block : (place + 1) * block] = (
                mixed[place] * scale_unit
            ).astype(jnp.bfloat16)
        return carry

    def band(index):
        return pl.ds(pl.multiple_of(index * sub, sub), sub)

    def fold_copy(column):
        return pltpu.make_async_remote_copy(
            src_ref=core_out.at[column],
            dst_ref=core_in.at[column],
            send_sem=fold_send.at[column],
            recv_sem=fold_recv.at[column],
            device_id={"tensor": partner},
            device_id_type=MESH,
        )

    def chip_copy(step, column):
        return pltpu.make_async_remote_copy(
            src_ref=chip_out.at[column, step],
            dst_ref=chip_in.at[column, step],
            send_sem=chip_send.at[step, column],
            recv_sem=chip_recv.at[step, column],
            device_id={"tensor": peer(step)},
            device_id_type=MESH,
        )

    def multiply(column):
        wave, nibble = column // NIBBLES, lax.rem(column, NIBBLES)
        sums[...] = jnp.dot(rotated[wave], weights[nibble], preferred_element_type=jnp.float32)
        for step in range(chips):
            target = lax.rem(chip + step, chips)
            core_out[column, target] = sums[band(target * 2 + 1 - core), :].astype(jnp.bfloat16)
            own[column, step] = sums[band(target * 2 + core), :]
        fold_copy(column).start()

    def fold(column):
        fold_copy(column).wait_recv()
        for step in range(1, chips):
            target = lax.rem(chip + step, chips)
            chip_out[column, step] = (
                own[column, step] + core_in[column, target].astype(jnp.float32)
            ).astype(jnp.bfloat16)
            chip_copy(step, column).start()
        own[column, 0] = own[column, 0] + core_in[column, chip].astype(jnp.float32)

    def column_step(column, carry):
        multiply(column)

        @pl.when(column > 0)
        def _():
            fold(column - 1)

        return carry

    for wave in range(waves):
        lax.fori_loop(wave * units, (wave + 1) * units, rotate, 0)
        lax.fori_loop(wave * NIBBLES, (wave + 1) * NIBBLES, column_step, 0)
    fold(waves * NIBBLES - 1)

    factor = 1.0 / (45.0 * math.sqrt(groups * width))
    for column in range(waves * NIBBLES):
        wave, nibble = column // NIBBLES, column % NIBBLES
        span = (slice(wave * sub, (wave + 1) * sub), slice(nibble * word_cols, (nibble + 1) * word_cols))
        total = own[column, 0]
        for step in range(1, chips):
            chip_copy(step, column).wait_recv()
            total += chip_in[column, step].astype(jnp.float32)
        new_residual[span] = (residual[span].astype(jnp.float32) + total * factor).astype(jnp.bfloat16)

    def drain_rows(unit, carry):
        for step in range(1, chips):
            peer_copy(step, unit).wait_send()
        for step in range(chips):
            core_copy(step, unit).wait_send()
        return carry

    for step in range(1, groups):
        sign_copy(step).wait_send()
    lax.fori_loop(0, groups, drain_rows, 0)

    def drain_columns(column, carry):
        fold_copy(column).wait_send()
        for step in range(1, chips):
            chip_copy(step, column).wait_send()
        return carry

    lax.fori_loop(0, waves * NIBBLES, drain_columns, 0)


def finish(fresh, new_residual, normed):
    values = fresh[...].astype(jnp.float32)
    new_residual[...] = fresh[...]
    inverse = lax.rsqrt(jnp.mean(values * values, axis=1, keepdims=True) + 1e-05)
    normed[...] = (values * inverse).astype(jnp.bfloat16)


def local(groups, hidden, signs, packed, group_scales, residual):
    rows, width = hidden.shape
    part = rows // groups
    chips = groups // 2
    waves = max(1, min(WAVES, part // SLAB, groups))
    word_cols = packed.shape[1]
    block = math.lcm(PALEY, LANES)
    table = np.kron(sylvester(block // PALEY), paley_table()).astype(ml_dtypes.bfloat16)
    vmem = pl.BlockSpec(memory_space=pltpu.VMEM)
    anywhere = pl.BlockSpec(memory_space=pl.ANY)
    dma = pltpu.SemaphoreType.DMA
    count = waves * NIBBLES
    tall = (count, chips, part // waves, word_cols)
    sign_shape = (width // LANES, LANES)
    out = jax.ShapeDtypeStruct(residual.shape, jnp.bfloat16)
    fresh = pl.pallas_call(
        functools.partial(kernel, groups, waves),
        out_shape=out,
        in_specs=[anywhere] * 6,
        out_specs=vmem,
        scratch_shapes=[
            pltpu.VMEM(group_scales.shape, jnp.int32),
            pltpu.VMEM(residual.shape, jnp.bfloat16),
            pltpu.VMEM(packed.shape, jnp.int32),
            pltpu.VMEM((block, block), jnp.bfloat16),
            pltpu.VMEM((groups, groups, part, width), jnp.bfloat16),
            pltpu.VMEM((groups,) + sign_shape, jnp.int32),
            pltpu.VMEM((groups,) + sign_shape, jnp.float32),
            pltpu.VMEM(group_scales.shape, jnp.float32),
            pltpu.VMEM((NIBBLES, width, word_cols), jnp.bfloat16),
            pltpu.VMEM((waves, rows // waves, width), jnp.bfloat16),
            pltpu.VMEM((rows // waves, word_cols), jnp.float32),
            pltpu.VMEM(tall, jnp.float32),
            pltpu.VMEM(tall, jnp.bfloat16),
            pltpu.VMEM(tall, jnp.bfloat16),
            pltpu.VMEM(tall, jnp.bfloat16),
            pltpu.VMEM(tall, jnp.bfloat16),
            dma,
            dma,
            dma,
            dma,
            dma,
            dma,
            dma((groups,)),
            dma((groups,)),
            dma((chips, groups)),
            dma((chips, groups)),
            dma((chips, groups)),
            dma((chips, groups)),
            dma((count,)),
            dma((count,)),
            dma((chips, count)),
            dma((chips, count)),
        ],
        compiler_params=pltpu.CompilerParams(
            collective_id=0, has_side_effects=True, vmem_limit_bytes=67043328
        ),
    )(
        hidden.reshape(groups, part, width),
        signs.reshape(sign_shape),
        packed,
        group_scales,
        jnp.asarray(table),
        residual,
    )
    return pl.pallas_call(
        finish,
        out_shape=(out, out),
        in_specs=[vmem],
        out_specs=(vmem, vmem),
    )(fresh)


def solution(mesh):
    return jax.shard_map(
        functools.partial(local, mesh.shape["tensor"]),
        mesh=mesh,
        in_specs=(
            P("dp", "tensor"),
            P("tensor"),
            P("tensor", None),
            P("tensor", None),
            P(("dp", "tensor"), None),
        ),
        out_specs=(P(("dp", "tensor"), None), P(("dp", "tensor"), None)),
        check_vma=False,
    )
```
